128 devices in a mesh: gx: 16 (over y, z_lo, core), gy: 8 (over z_hi, x).
Axes of the slice: x: 4, y: 4, z: 4 (z_hi: 2, z_lo: 2; z = z_hi * 2 + z_lo), core: 2. Of those that a mesh axis runs over, the one named last changes fastest.
Arguments:
- kernels: bfloat16 [4, 4, 1024, 512, 128], P(None, None, 'gx', 'gy'), may hold values from -600 to 600
- event_weight: float32 [4], replicated, may hold values from 0.3 to 3
Outputs:
- smoothed: float32 [4, 1024, 512, 128], P(None, 'gx', 'gy')
The draws below stay inside these ranges and needn't reach their ends.
All inputs are finite; a program needn't handle non-finite values.
Results may differ from the reference program's by a relative error of at most 0.0053.
Values may be sent and summed in bfloat16 or wider, within the bound.
No kernel may reach another device: no remote copies, remote signals or barrier semaphores. Data moves between devices by JAX's collectives and lax.ppermute only.
A program may use at most 192 MiB of HBM per device.

```python
import math
import jax
import jax.numpy as jnp

BLOCK = 64
DEPTH = 128
PARAMS = 4
EVENTS = 4
RADIUS = 192
NX = 1024
NY = 512


def block_scale(rng, extent, shards, smallest, high):
    gain, own = 1.0, jax.random.fold_in(rng, 6)
    for position, shards_of in shards:
        steps = jnp.exp(jax.random.uniform(jax.random.fold_in(own, position), (shards_of,), jnp.float32, smallest / len(shards), high / len(shards)))
        gain = gain * jnp.repeat(steps, extent[position] // shards_of).reshape([-1 if axis == position else 1 for axis in range(len(extent))])
    return gain


def gaussian(key, extent, deviation, bound, cuts=(), held_as=jnp.bfloat16):
    factor_of = block_scale(key, extent, cuts, -0.22, 0.18) if cuts else 1.0
    entries = jax.random.normal(key, extent, jnp.float32) * deviation * factor_of
    return jnp.minimum(jnp.maximum(entries, -bound), bound).astype(held_as)


def setup_inputs(seed: int = 0) -> dict:
    streams_of = jax.random.split(jax.random.key(seed), 3)
    return {
        "kernels": gaussian(streams_of[0], (EVENTS, PARAMS, NX, NY, DEPTH), 100.0, 600.0, ((2, 16), (3, 8))),
        "event_weight": jnp.clip(jnp.exp(jax.random.uniform(streams_of[1], (EVENTS,), jnp.float32, math.log(0.3), math.log(3.0))), 0.3, 3.0),
    }


def band_matrix(count, radius, sigma):
    rows = jnp.arange(count, dtype=jnp.int32)
    offsets = rows[None, :] - rows[:, None]
    values = offsets.astype(jnp.float32)
    weights = jnp.exp(-values * values / (2.0 * sigma * sigma))
    return jnp.where(jnp.abs(offsets) <= radius, weights, 0.0).astype(jnp.bfloat16)


def reference(kernels, event_weight):
    sigma = 2.0 * BLOCK
    summed = jnp.sum(event_weight[:, None, None, None, None] * kernels.astype(jnp.float32), axis=0).astype(jnp.bfloat16)
    mat_x = band_matrix(NX, RADIUS, sigma)
    norm_x = jnp.sum(mat_x.astype(jnp.float32), axis=1)
    flat = jnp.moveaxis(summed, 1, 0).reshape(NX, -1)
    along_x = jnp.dot(mat_x, flat, preferred_element_type=jnp.float32) / norm_x[:, None]
    along_x = along_x.astype(jnp.bfloat16).reshape(NX, PARAMS, NY, DEPTH)
    mat_y = band_matrix(NY, RADIUS, sigma)
    norm_y = jnp.sum(mat_y.astype(jnp.float32), axis=1)
    flat_y = jnp.moveaxis(along_x, 2, 0).reshape(NY, -1)
    result = jnp.dot(mat_y, flat_y, preferred_element_type=jnp.float32) / norm_y[:, None]
    result = result.reshape(NY, NX, PARAMS, DEPTH)
    result = jnp.moveaxis(result, 0, 2)
    return jnp.moveaxis(result, 1, 0)
```

```python
import functools
import jax
import jax.numpy as jnp
from jax import lax
from jax.experimental import pallas as pl
from jax.experimental.pallas import tpu as pltpu
from jax.sharding import PartitionSpec as P

REACH = 3
AXES = ("gx", "gy")
ROWS = 8


def gauss_weights(offsets, radius, sigma):
    values = offsets.astype(jnp.float32)
    weights = jnp.exp(-values * values / (2.0 * sigma * sigma))
    return jnp.where(jnp.abs(offsets) <= radius, weights, 0.0).astype(jnp.bfloat16)


def inverse_norms(total, radius, sigma):
    steps = jnp.arange(-radius, radius + 1, dtype=jnp.int32)
    places = jnp.arange(total, dtype=jnp.int32)[:, None] + steps[None, :]
    table = gauss_weights(steps, radius, sigma).astype(jnp.float32)
    inside = (places >= 0) & (places < total)
    return 1.0 / jnp.sum(jnp.where(inside, table[None, :], 0.0), axis=1)


def sum_kernel(weight_ref, kernels_ref, out_ref, turned):
    events, _, halves, rows, width, depth = kernels_ref.shape
    for r in range(rows):
        parts = []
        for h in range(halves):
            total = weight_ref[0] * kernels_ref[0, 0, h, r].astype(jnp.float32)
            for e in range(1, events):
                total = total + weight_ref[e] * kernels_ref[e, 0, h, r].astype(jnp.float32)
            parts.append(total)
        turned[pl.ds(r, depth, stride=rows), :] = jnp.concatenate(parts, axis=0).T
    out_ref[:, 0] = turned[...].reshape(depth, rows, halves * width).astype(out_ref.dtype)


def event_sum(kernels, event_weight):
    events, params, nx, ny, depth = kernels.shape
    halves = depth // ny
    split = kernels.reshape(events, params, halves, nx // halves, ny, depth)
    return pl.pallas_call(
        sum_kernel,
        grid=(params, nx // halves // ROWS),
        in_specs=[
            pl.BlockSpec(memory_space=pltpu.SMEM),
            pl.BlockSpec((events, 1, halves, ROWS, ny, depth), lambda p, r: (0, p, 0, r, 0, 0)),
        ],
        out_specs=pl.BlockSpec((depth, 1, ROWS, halves * ny), lambda p, r: (0, p, r, 0)),
        out_shape=jax.ShapeDtypeStruct((depth, params, nx // halves, halves * ny), jnp.bfloat16),
        scratch_shapes=[pltpu.VMEM((depth * ROWS, halves * ny), jnp.float32)],
        name="event_sum",
    )(event_weight, split)


def smooth_kernel(size_y, block, in_ref, tile_ref, tile_t_ref, inv_x_ref, inv_y_ref, out_ref, plane):
    nx, ny = plane.shape
    rows = in_ref.shape[2]
    tile, reach = tile_ref.shape[0], REACH * block
    pair = 2 * block

    @pl.loop(0, nx // block)
    def _(i):
        for j in range(0, size_y, 2):
            a, b = in_ref[i * size_y + j, 0], in_ref[i * size_y + j + 1, 0]
            cols = pl.ds(j * block, pair)
            plane[pl.ds(i * block, rows), cols] = jnp.concatenate([a[:, :block], b[:, :block]], axis=1)
            plane[pl.ds(i * block + rows, rows), cols] = jnp.concatenate([a[:, block:], b[:, block:]], axis=1)

    for x0 in range(0, nx, tile):
        lo, hi = max(0, x0 - reach), min(nx, x0 + tile + reach)
        at = lo - (x0 - reach)
        sums = jnp.dot(tile_ref[:, at : at + hi - lo], plane[lo:hi], preferred_element_type=jnp.float32)
        along_x = (sums * inv_x_ref[x0 : x0 + tile]).astype(jnp.bfloat16)
        for y0 in range(0, ny, tile):
            lo, hi = max(0, y0 - reach), min(ny, y0 + tile + reach)
            at = lo - (y0 - reach)
            sums = jnp.dot(along_x[:, lo:hi], tile_t_ref[at : at + hi - lo], preferred_element_type=jnp.float32)
            done = (sums * inv_y_ref[:, y0 : y0 + tile]).astype(jnp.bfloat16)
            for i in range(tile // block):
                for j in range(0, tile // block, 2):
                    part = done[i * block : (i + 1) * block, j * block : j * block + pair]
                    a, b = part[:rows], part[rows:]
                    at_block = (x0 // block + i) * size_y + y0 // block + j
                    out_ref[at_block, 0] = jnp.concatenate([a[:, :block], b[:, :block]], axis=1)
                    out_ref[at_block + 1, 0] = jnp.concatenate([a[:, block:], b[:, block:]], axis=1)


def smooth(lines, block, size_x, size_y, tables):
    blocks, params, rows, width = lines.shape
    nx, ny = size_x * block, size_y * block
    whole = lambda a: pl.BlockSpec(a.shape, lambda p: (0,) * a.ndim)
    spec = pl.BlockSpec((blocks, 1, rows, width), lambda p: (0, p, 0, 0))
    return pl.pallas_call(
        functools.partial(smooth_kernel, size_y, block),
        grid=(params,),
        in_specs=[spec] + [whole(t) for t in tables],
        out_specs=spec,
        out_shape=jax.ShapeDtypeStruct(lines.shape, jnp.bfloat16),
        scratch_shapes=[pltpu.VMEM((nx, ny), jnp.bfloat16)],
        name="smooth",
    )(lines, *tables)


def turn_kernel(in_ref, out_ref, wide):
    depth, _, rows, pair = in_ref.shape
    halves, width = out_ref.shape[1], out_ref.shape[3]
    wide[...] = in_ref[:, 0].astype(jnp.float32).reshape(depth * rows, pair)
    for r in range(rows):
        turned = wide[pl.ds(r, depth, stride=rows), :].T
        for h in range(halves):
            out_ref[0, h, r] = turned[h * width : (h + 1) * width]


def turn_back(done, block):
    depth, params, rows, pair = done.shape
    halves = pair // block
    out = pl.pallas_call(
        turn_kernel,
        grid=(params, rows // ROWS),
        in_specs=[pl.BlockSpec((depth, 1, ROWS, pair), lambda p, r: (0, p, r, 0))],
        out_specs=pl.BlockSpec((1, halves, ROWS, block, depth), lambda p, r: (p, 0, r, 0, 0)),
        out_shape=jax.ShapeDtypeStruct((params, halves, rows, block, depth), jnp.float32),
        scratch_shapes=[pltpu.VMEM((depth * ROWS, pair), jnp.float32)],
        name="turn_back",
    )(done)
    return out.reshape(params, halves * rows, block, depth)


def body(kernels, event_weight):
    block = kernels.shape[2]
    radius, sigma = REACH * block, 2.0 * block
    size_x, size_y = lax.axis_size("gx"), lax.axis_size("gy")
    tile = 4 * block
    offsets = jnp.arange(tile + 2 * radius)[None, :] - jnp.arange(tile)[:, None] - radius
    tables = (
        gauss_weights(offsets, radius, sigma),
        gauss_weights(offsets.T, radius, sigma),
        inverse_norms(size_x * block, radius, sigma)[:, None],
        inverse_norms(size_y * block, radius, sigma)[None, :],
    )
    summed = event_sum(kernels, event_weight)
    planes = lax.all_to_all(summed, AXES, split_axis=0, concat_axis=0, tiled=True)
    done = smooth(planes, block, size_x, size_y, tables)
    blocks = lax.all_to_all(done, AXES, split_axis=0, concat_axis=0, tiled=True)
    return turn_back(blocks, block)


def solution(mesh):
    return jax.shard_map(
        body,
        mesh=mesh,
        in_specs=(P(None, None, "gx", "gy", None), P()),
        out_specs=P(None, "gx", "gy", None),
        check_vma=False,
    )
```

```python
import functools
import jax
import jax.numpy as jnp
from jax import lax
from jax.experimental import pallas as pl
from jax.experimental.pallas import tpu as pltpu
from jax.sharding import PartitionSpec as P

REACH = 3
AXES = ("gx", "gy")
TILE = 4
SUM_MIB = 36
ROWS = 8


def gauss_weights(offsets, radius, sigma):
    values = offsets.astype(jnp.float32)
    weights = jnp.exp(-values * values / (2.0 * sigma * sigma))
    return jnp.where(jnp.abs(offsets) <= radius, weights, 0.0).astype(jnp.bfloat16)


def band(rows, cols, shift, axis, sigma, radius):
    far = lax.broadcasted_iota(jnp.int32, (rows, cols), axis)
    near = lax.broadcasted_iota(jnp.int32, (rows, cols), 1 - axis)
    return gauss_weights(far - near - shift, radius, sigma)


def sum_kernel(block, weight_ref, kernels_ref, out_ref, tile_ref, tile_t_ref, inv_x_ref, inv_y_ref, landing, turned, arrived):
    steps, events, halves, rows, width, depth = landing.shape
    per_param = steps // kernels_ref.shape[1]
    radius, sigma = REACH * block, 2.0 * block

    def copy(s):
        p, r = s // per_param, lax.rem(s, per_param)
        return pltpu.make_async_copy(
            kernels_ref.at[:, p, :, pl.ds(r * rows, rows)], landing.at[s], arrived.at[s]
        )

    @pl.loop(0, steps)
    def _(s):
        copy(s).start()

    tile, reach = tile_ref.shape
    weights = band(tile, reach, radius, 1, sigma, radius)
    tile_ref[...] = weights
    weights_t = band(reach, tile, radius, 0, sigma, radius)
    tile_t_ref[...] = weights_t
    nx, ny = inv_x_ref.shape[0], inv_y_ref.shape[1]
    for x0 in range(0, nx, tile):
        lo, hi = clipped(x0, tile, radius, nx)
        sums = jnp.sum(weights[:, lo:hi].astype(jnp.float32), axis=1, keepdims=True)
        inv_x_ref[x0 : x0 + tile] = jnp.broadcast_to(1.0 / sums, (tile, inv_x_ref.shape[1]))
    for y0 in range(0, ny, tile):
        lo, hi = clipped(y0, tile, radius, ny)
        sums = jnp.sum(weights_t[lo:hi].astype(jnp.float32), axis=0, keepdims=True)
        inv_y_ref[:, y0 : y0 + tile] = jnp.broadcast_to(1.0 / sums, (inv_y_ref.shape[0], tile))

    @pl.loop(0, steps)
    def _(s):
        copy(s).wait()
        for r in range(rows):
            parts = []
            for h in range(halves):
                total = weight_ref[0] * landing[s, 0, h, r].astype(jnp.float32)
                for e in range(1, events):
                    total = total + weight_ref[e] * landing[s, e, h, r].astype(jnp.float32)
                parts.append(total)
            turned[pl.ds(r, depth, stride=rows), :] = jnp.concatenate(parts, axis=0).T
        p, place = s // per_param, pl.multiple_of(lax.rem(s, per_param) * rows, rows)
        whole = turned[...].reshape(depth, rows, halves * width)
        out_ref[:, p, pl.ds(place, rows)] = whole.astype(out_ref.dtype)


def clipped(first, tile, radius, total):
    return max(0, radius - first), min(tile + 2 * radius, total - first + radius)


def event_sum(kernels, event_weight, nx_all, ny_all):
    events, params, nx, ny, depth = kernels.shape
    halves = depth // ny
    rows = nx // halves
    split = kernels.reshape(events, params, halves, rows, ny, depth)
    tile, reach = TILE * nx, (TILE + 2 * REACH) * nx
    steps = params * rows // ROWS
    vmem = pl.BlockSpec(memory_space=pltpu.VMEM)
    return pl.pallas_call(
        functools.partial(sum_kernel, nx),
        in_specs=[pl.BlockSpec(memory_space=pltpu.SMEM), pl.BlockSpec(memory_space=pl.ANY)],
        out_specs=(vmem,) * 5,
        out_shape=(
            jax.ShapeDtypeStruct((depth, params, rows, halves * ny), jnp.bfloat16),
            jax.ShapeDtypeStruct((tile, reach), jnp.bfloat16),
            jax.ShapeDtypeStruct((reach, tile), jnp.bfloat16),
            jax.ShapeDtypeStruct((nx_all, depth), jnp.float32),
            jax.ShapeDtypeStruct((8, ny_all), jnp.float32),
        ),
        scratch_shapes=[
            pltpu.VMEM((steps, events, halves, ROWS, ny, depth), jnp.bfloat16),
            pltpu.VMEM((depth * ROWS, halves * ny), jnp.float32),
            pltpu.SemaphoreType.DMA((steps,)),
        ],
        compiler_params=pltpu.CompilerParams(vmem_limit_bytes=SUM_MIB << 20),
        name="event_sum",
    )(event_weight, split)


def smooth_kernel(size_y, block, in_ref, tile_ref, tile_t_ref, inv_x_ref, inv_y_ref, out_ref, plane):
    nx, ny = plane.shape
    rows = in_ref.shape[2]
    tile, reach = tile_ref.shape[0], REACH * block
    pair = 2 * block

    def build(i):
        for j in range(0, size_y, 2):
            a, b = in_ref[i * size_y + j, 0], in_ref[i * size_y + j + 1, 0]
            cols = slice(j * block, j * block + pair)
            plane[i * block : i * block + rows, cols] = jnp.concatenate([a[:, :block], b[:, :block]], axis=1)
            plane[i * block + rows : (i + 1) * block, cols] = jnp.concatenate([a[:, block:], b[:, block:]], axis=1)

    built = 0
    for x0 in range(0, nx, tile):
        lo, hi = max(0, x0 - reach), min(nx, x0 + tile + reach)
        while built * block < hi:
            build(built)
            built += 1
        at = lo - (x0 - reach)
        sums = jnp.dot(tile_ref[:, at : at + hi - lo], plane[lo:hi], preferred_element_type=jnp.float32)
        inv_x = jnp.concatenate([inv_x_ref[x0 : x0 + tile]] * (ny // inv_x_ref.shape[1]), axis=1)
        along_x = (sums * inv_x).astype(jnp.bfloat16)
        for y0 in range(0, ny, tile):
            lo, hi = max(0, y0 - reach), min(ny, y0 + tile + reach)
            at = lo - (y0 - reach)
            sums = jnp.dot(along_x[:, lo:hi], tile_t_ref[at : at + hi - lo], preferred_element_type=jnp.float32)
            done = (sums * inv_y_ref[0:1, y0 : y0 + tile]).astype(jnp.bfloat16)
            for i in range(tile // block):
                for j in range(0, tile // block, 2):
                    part = done[i * block : (i + 1) * block, j * block : j * block + pair]
                    a, b = part[:rows], part[rows:]
                    at_block = (x0 // block + i) * size_y + y0 // block + j
                    out_ref[at_block, 0] = jnp.concatenate([a[:, :block], b[:, :block]], axis=1)
                    out_ref[at_block + 1, 0] = jnp.concatenate([a[:, block:], b[:, block:]], axis=1)


def smooth(lines, block, size_x, size_y, tables):
    blocks, params, rows, width = lines.shape
    nx, ny = size_x * block, size_y * block
    whole = lambda a: pl.BlockSpec(a.shape, lambda p: (0,) * a.ndim)
    spec = pl.BlockSpec((blocks, 1, rows, width), lambda p: (0, p, 0, 0))
    return pl.pallas_call(
        functools.partial(smooth_kernel, size_y, block),
        grid=(params,),
        in_specs=[spec] + [whole(t) for t in tables],
        out_specs=spec,
        out_shape=jax.ShapeDtypeStruct(lines.shape, jnp.bfloat16),
        scratch_shapes=[pltpu.VMEM((nx, ny), jnp.bfloat16)],
        compiler_params=pltpu.CompilerParams(vmem_limit_bytes=16 << 20),
        name="smooth",
    )(lines, *tables)


def turn_kernel(in_ref, out_ref, leaving, wide, left):
    steps, halves, rows, width, _ = leaving.shape
    depth, params, _, pair = in_ref.shape
    per_param = steps // params

    def copy(s):
        p, r = s // per_param, lax.rem(s, per_param)
        return pltpu.make_async_copy(leaving.at[s], out_ref.at[p, :, pl.ds(r * rows, rows)], left.at[s])

    @pl.loop(0, steps)
    def _(s):
        p, place = s // per_param, pl.multiple_of(lax.rem(s, per_param) * rows, rows)
        wide[...] = in_ref[:, p, pl.ds(place, rows)].astype(jnp.float32).reshape(depth * rows, pair)
        for r in range(rows):
            turned = wide[pl.ds(r, depth, stride=rows), :].T
            for h in range(halves):
                leaving[s, h, r] = turned[h * width : (h + 1) * width]
        copy(s).start()

    @pl.loop(0, steps)
    def _(s):
        copy(s).wait()


def turn_back(done, block):
    depth, params, rows, pair = done.shape
    halves = pair // block
    steps = params * rows // ROWS
    out = pl.pallas_call(
        turn_kernel,
        in_specs=[pl.BlockSpec(memory_space=pltpu.VMEM)],
        out_specs=pl.BlockSpec(memory_space=pl.ANY),
        out_shape=jax.ShapeDtypeStruct((params, halves, rows, block, depth), jnp.float32),
        scratch_shapes=[
            pltpu.VMEM((steps, halves, ROWS, block, depth), jnp.float32),
            pltpu.VMEM((depth * ROWS, pair), jnp.float32),
            pltpu.SemaphoreType.DMA((steps,)),
        ],
        compiler_params=pltpu.CompilerParams(vmem_limit_bytes=24 << 20),
        name="turn_back",
    )(done)
    return out.reshape(params, halves * rows, block, depth)


def body(kernels, event_weight):
    block = kernels.shape[2]
    size_x, size_y = lax.axis_size("gx"), lax.axis_size("gy")
    summed, *tables = event_sum(kernels, event_weight, size_x * block, size_y * block)
    swap = functools.partial(lax.all_to_all, axis_name=AXES, split_axis=0, concat_axis=0, tiled=True)
    done = smooth(swap(summed), block, size_x, size_y, tables)
    return turn_back(swap(done), block)


def solution(mesh):
    return jax.shard_map(
        body,
        mesh=mesh,
        in_specs=(P(None, None, "gx", "gy", None), P()),
        out_specs=P(None, "gx", "gy", None),
        check_vma=False,
    )
```

```python
import functools
import jax
import jax.numpy as jnp
from jax import lax
from jax.experimental import pallas as pl
from jax.experimental.pallas import tpu as pltpu
from jax.sharding import PartitionSpec as P

REACH = 3
MARGIN = 4
AXES = ("gx", "gy")
TILE = 8
SUM_MIB = 36
SMOOTH_MIB = 24
PLANES = 4
SUM_UNROLL = 2
TURN_UNROLL = 4
ROWS = 8


def gauss_weights(offsets, radius, sigma):
    values = offsets.astype(jnp.float32)
    weights = jnp.exp(-values * values / (2.0 * sigma * sigma))
    return jnp.where(jnp.abs(offsets) <= radius, weights, 0.0).astype(jnp.bfloat16)


def band(rows, cols, shift, axis, sigma, radius):
    far = lax.broadcasted_iota(jnp.int32, (rows, cols), axis)
    near = lax.broadcasted_iota(jnp.int32, (rows, cols), 1 - axis)
    return gauss_weights(far - near - shift, radius, sigma)


def clipped(first, window, margin, total):
    return max(0, margin - first), min(window, total - first + margin)


def make_tables(block, tile_ref, tile_t_ref, inv_x_ref, inv_y_ref):
    radius, sigma, margin = REACH * block, 2.0 * block, MARGIN * block
    step = 2 * block
    window = step + 2 * margin
    weights = band(step, window, margin, 1, sigma, radius)
    weights_t = band(window, step, margin, 0, sigma, radius)
    tile, reach = tile_ref.shape
    for at in range(0, tile, step):
        own = slice(at, at + step)
        tile_ref[own, at : at + window] = weights
        tile_t_ref[at : at + window, own] = weights_t
        for lo, hi in ((0, at), (at + window, reach)):
            if hi > lo:
                tile_ref[own, lo:hi] = jnp.zeros((step, hi - lo), tile_ref.dtype)
                tile_t_ref[lo:hi, own] = jnp.zeros((hi - lo, step), tile_t_ref.dtype)
    nx, ny = inv_x_ref.shape[0], inv_y_ref.shape[1]
    wide, wide_t = weights.astype(jnp.float32), weights_t.astype(jnp.float32)
    for x0 in range(0, nx, step):
        lo, hi = clipped(x0, window, margin, nx)
        sums = jnp.sum(wide[:, lo:hi], axis=1, keepdims=True)
        inv_x_ref[x0 : x0 + step] = jnp.broadcast_to(1.0 / sums, (step, inv_x_ref.shape[1]))
    for y0 in range(0, ny, step):
        lo, hi = clipped(y0, window, margin, ny)
        sums = jnp.sum(wide_t[lo:hi], axis=0, keepdims=True)
        inv_y_ref[:, y0 : y0 + step] = jnp.broadcast_to(1.0 / sums, (inv_y_ref.shape[0], step))


def sum_kernel(block, weight_hbm, kernels_ref, out_ref, *refs):
    tables, (landing, weight_ref, turned, arrived, weighed) = refs[:4], refs[4:]
    steps, events, halves, rows, width, depth = landing.shape
    per_param = steps // kernels_ref.shape[1]

    def copy(s):
        p, r = s // per_param, lax.rem(s, per_param)
        return pltpu.make_async_copy(
            kernels_ref.at[:, p, :, pl.ds(r * rows, rows)], landing.at[s], arrived.at[s]
        )

    weigh = pltpu.make_async_copy(weight_hbm, weight_ref, weighed)
    weigh.start()

    @pl.loop(0, steps)
    def _(s):
        copy(s).start()

    make_tables(block, *tables)
    weigh.wait()
    weight = [weight_ref[e] for e in range(events)]

    @pl.loop(0, steps, step=SUM_UNROLL)
    def _(first):
        for u in range(SUM_UNROLL):
            s = first + u
            copy(s).wait()
            for r in range(rows):
                parts = []
                for h in range(halves):
                    total = weight[0] * landing[s, 0, h, r].astype(jnp.float32)
                    for e in range(1, events):
                        total = total + weight[e] * landing[s, e, h, r].astype(jnp.float32)
                    parts.append(total)
                turned[u, pl.ds(r, depth, stride=rows), :] = jnp.concatenate(parts, axis=0).T
            p, place = s // per_param, pl.multiple_of(lax.rem(s, per_param) * rows, rows)
            whole = turned[u].reshape(depth, rows, halves * width)
            out_ref[:, p, pl.ds(place, rows)] = whole.astype(out_ref.dtype)


def event_sum(kernels, event_weight, nx_all, ny_all):
    events, params, nx, ny, depth = kernels.shape
    halves = depth // ny
    rows = nx // halves
    split = kernels.reshape(events, params, halves, rows, ny, depth)
    tile, reach = TILE * nx, (TILE + 2 * MARGIN) * nx
    steps = params * rows // ROWS
    vmem = pl.BlockSpec(memory_space=pltpu.VMEM)
    hbm = pl.BlockSpec(memory_space=pltpu.HBM)
    return pl.pallas_call(
        functools.partial(sum_kernel, nx),
        in_specs=[hbm, hbm],
        out_specs=(vmem,) * 5,
        out_shape=(
            jax.ShapeDtypeStruct((depth, params, rows, halves * ny), jnp.bfloat16),
            jax.ShapeDtypeStruct((tile, reach), jnp.bfloat16),
            jax.ShapeDtypeStruct((reach, tile), jnp.bfloat16),
            jax.ShapeDtypeStruct((nx_all, depth), jnp.float32),
            jax.ShapeDtypeStruct((8, ny_all), jnp.float32),
        ),
        scratch_shapes=[
            pltpu.VMEM((steps, events, halves, ROWS, ny, depth), jnp.bfloat16),
            pltpu.SMEM((events,), jnp.float32),
            pltpu.VMEM((SUM_UNROLL, depth * ROWS, halves * ny), jnp.float32),
            pltpu.SemaphoreType.DMA((steps,)),
            pltpu.SemaphoreType.DMA,
        ],
        compiler_params=pltpu.CompilerParams(vmem_limit_bytes=SUM_MIB << 20),
        name="event_sum",
    )(pltpu.with_memory_space_constraint(event_weight, pltpu.HBM), split)


def smooth_kernel(size_y, block, in_ref, tile_ref, tile_t_ref, inv_x_ref, inv_y_ref, out_ref, plane):
    _, pairs, nx, pair = plane.shape
    ny = pairs * pair
    rows = in_ref.shape[2]
    tile, reach = tile_ref.shape[0], MARGIN * block
    swap_halves = lambda a, b: (
        jnp.concatenate([a[:, :block], b[:, :block]], axis=1),
        jnp.concatenate([a[:, block:], b[:, block:]], axis=1),
    )

    def build(p, i):
        for j in range(pairs):
            at = i * size_y + 2 * j
            upper, lower = swap_halves(in_ref[at, p], in_ref[at + 1, p])
            plane[p, j, i * block : i * block + rows] = upper
            plane[p, j, i * block + rows : (i + 1) * block] = lower

    def build_for(p, x0):
        first = 0 if x0 == 0 else min(nx, x0 + reach) // block
        for i in range(first, min(nx, x0 + tile + reach) // block):
            build(p, i)

    def pack(p, x0, done):
        for i in range(tile // block):
            for j in range(0, size_y, 2):
                part = done[i * block : (i + 1) * block, j * block : j * block + pair]
                at = (x0 // block + i) * size_y + j
                out_ref[at, p], out_ref[at + 1, p] = swap_halves(part[:rows], part[rows:])

    jobs = [(p, x0) for p in range(in_ref.shape[1]) for x0 in range(0, nx, tile)]
    build_for(*jobs[0])
    last = None
    for k, (p, x0) in enumerate(jobs):
        lo, hi = max(0, x0 - reach), min(nx, x0 + tile + reach)
        at = lo - (x0 - reach)
        lines = jnp.concatenate([plane[p, j, lo:hi] for j in range(pairs)], axis=1)
        sums = jnp.dot(tile_ref[:, at : at + hi - lo], lines, preferred_element_type=jnp.float32)
        if k + 1 < len(jobs):
            build_for(*jobs[k + 1])
        inv_x = jnp.concatenate([inv_x_ref[x0 : x0 + tile]] * (ny // inv_x_ref.shape[1]), axis=1)
        along_x = (sums * inv_x).astype(jnp.bfloat16)
        if last is not None:
            pack(*last)
        parts = []
        for y0 in range(0, ny, tile):
            lo, hi = max(0, y0 - reach), min(ny, y0 + tile + reach)
            at = lo - (y0 - reach)
            sums = jnp.dot(along_x[:, lo:hi], tile_t_ref[at : at + hi - lo], preferred_element_type=jnp.float32)
            parts.append((sums * inv_y_ref[0:1, y0 : y0 + tile]).astype(jnp.bfloat16))
        last = p, x0, jnp.concatenate(parts, axis=1)
    pack(*last)


def smooth(lines, block, size_x, size_y, tables):
    blocks, params, rows, width = lines.shape
    nx = size_x * block
    whole = lambda a: pl.BlockSpec(a.shape, lambda p: (0,) * a.ndim)
    spec = pl.BlockSpec((blocks, PLANES, rows, width), lambda p: (0, p, 0, 0))
    return pl.pallas_call(
        functools.partial(smooth_kernel, size_y, block),
        grid=(params // PLANES,),
        in_specs=[spec] + [whole(t) for t in tables],
        out_specs=spec,
        out_shape=jax.ShapeDtypeStruct(lines.shape, jnp.bfloat16),
        scratch_shapes=[pltpu.VMEM((PLANES, size_y // 2, nx, 2 * block), jnp.bfloat16)],
        compiler_params=pltpu.CompilerParams(vmem_limit_bytes=SMOOTH_MIB << 20),
        name="smooth",
    )(lines, *tables)


def turn_kernel(in_ref, out_ref, leaving, wide, left):
    steps, halves, rows, width, _ = leaving.shape
    depth, params, _, pair = in_ref.shape
    per_param = steps // params

    def copy(s):
        p, r = s // per_param, lax.rem(s, per_param)
        return pltpu.make_async_copy(leaving.at[s], out_ref.at[p, :, pl.ds(r * rows, rows)], left.at[s])

    @pl.loop(0, steps, step=TURN_UNROLL)
    def _(first):
        for u in range(TURN_UNROLL):
            s = first + u
            p, place = s // per_param, pl.multiple_of(lax.rem(s, per_param) * rows, rows)
            wide[u] = in_ref[:, p, pl.ds(place, rows)].astype(jnp.float32).reshape(depth * rows, pair)
            for r in range(rows):
                turned = wide[u, pl.ds(r, depth, stride=rows), :].T
                for h in range(halves):
                    leaving[s, h, r] = turned[h * width : (h + 1) * width]
            copy(s).start()

    @pl.loop(0, steps)
    def _(s):
        copy(s).wait()


def turn_back(done, block):
    depth, params, rows, pair = done.shape
    halves = pair // block
    steps = params * rows // ROWS
    out = pl.pallas_call(
        turn_kernel,
        in_specs=[pl.BlockSpec(memory_space=pltpu.VMEM)],
        out_specs=pl.BlockSpec(memory_space=pl.ANY),
        out_shape=jax.ShapeDtypeStruct((params, halves, rows, block, depth), jnp.float32),
        scratch_shapes=[
            pltpu.VMEM((steps, halves, ROWS, block, depth), jnp.float32),
            pltpu.VMEM((TURN_UNROLL, depth * ROWS, pair), jnp.float32),
            pltpu.SemaphoreType.DMA((steps,)),
        ],
        compiler_params=pltpu.CompilerParams(vmem_limit_bytes=24 << 20),
        name="turn_back",
    )(done)
    return out.reshape(params, halves * rows, block, depth)


def body(kernels, event_weight):
    block = kernels.shape[2]
    size_x, size_y = lax.axis_size("gx"), lax.axis_size("gy")
    summed, *tables = event_sum(kernels, event_weight, size_x * block, size_y * block)
    swap = functools.partial(lax.all_to_all, axis_name=AXES, split_axis=0, concat_axis=0, tiled=True)
    done = smooth(swap(summed), block, size_x, size_y, tables)
    return turn_back(swap(done), block)


def solution(mesh):
    return jax.shard_map(
        body,
        mesh=mesh,
        in_specs=(P(None, None, "gx", "gy", None), P()),
        out_specs=P(None, "gx", "gy", None),
        check_vma=False,
    )
```

```python
import functools
import jax
import jax.numpy as jnp
from jax import lax
from jax.experimental import pallas as pl
from jax.experimental.pallas import tpu as pltpu
from jax.sharding import PartitionSpec as P

REACH = 3
MARGIN = 4
AXES = ("gx", "gy")
TILE = 8
X_TILES = (5, 6, 5)
SUM_MIB = 36
SMOOTH_MIB = 24
PLANES = 4
SUM_UNROLL = 2
TURN_UNROLL = 16
ROWS = 8


def gauss_weights(offsets, radius, sigma):
    values = offsets.astype(jnp.float32)
    weights = jnp.exp(-values * values / (2.0 * sigma * sigma))
    return jnp.where(jnp.abs(offsets) <= radius, weights, 0.0).astype(jnp.bfloat16)


def band(rows, cols, shift, axis, sigma, radius):
    far = lax.broadcasted_iota(jnp.int32, (rows, cols), axis)
    near = lax.broadcasted_iota(jnp.int32, (rows, cols), 1 - axis)
    return gauss_weights(far - near - shift, radius, sigma)


def clipped(first, window, margin, total):
    return max(0, margin - first), min(window, total - first + margin)


def make_tables(block, tile_ref, tile_t_ref, inv_x_ref, inv_y_ref):
    radius, sigma, margin = REACH * block, 2.0 * block, MARGIN * block
    step = 2 * block
    window = step + 2 * margin
    weights = band(step, window, margin, 1, sigma, radius)
    weights_t = band(window, step, margin, 0, sigma, radius)
    tile, reach = tile_ref.shape
    for at in range(0, tile, step):
        own = slice(at, at + step)
        tile_ref[own, at : at + window] = weights
        tile_t_ref[at : at + window, own] = weights_t
        for lo, hi in ((0, at), (at + window, reach)):
            if hi > lo:
                tile_ref[own, lo:hi] = jnp.zeros((step, hi - lo), tile_ref.dtype)
                tile_t_ref[lo:hi, own] = jnp.zeros((hi - lo, step), tile_t_ref.dtype)
    nx, ny = inv_x_ref.shape[0], inv_y_ref.shape[1]
    wide, wide_t = weights.astype(jnp.float32), weights_t.astype(jnp.float32)
    for x0 in range(0, nx, step):
        lo, hi = clipped(x0, window, margin, nx)
        sums = jnp.sum(wide[:, lo:hi], axis=1, keepdims=True)
        inv_x_ref[x0 : x0 + step] = jnp.broadcast_to(1.0 / sums, (step, inv_x_ref.shape[1]))
    for y0 in range(0, ny, step):
        lo, hi = clipped(y0, window, margin, ny)
        sums = jnp.sum(wide_t[lo:hi], axis=0, keepdims=True)
        inv_y_ref[:, y0 : y0 + step] = jnp.broadcast_to(1.0 / sums, (inv_y_ref.shape[0], step))


def sum_kernel(block, weight_hbm, kernels_ref, out_ref, *refs):
    tables, (landing, weight_ref, turned, arrived, weighed) = refs[:4], refs[4:]
    steps, events, halves, rows, width, depth = landing.shape
    per_param = steps // kernels_ref.shape[1]

    def copy(s):
        p, r = s // per_param, lax.rem(s, per_param)
        return pltpu.make_async_copy(
            kernels_ref.at[:, p, :, pl.ds(r * rows, rows)], landing.at[s], arrived.at[s]
        )

    weigh = pltpu.make_async_copy(weight_hbm, weight_ref, weighed)
    weigh.start()

    @pl.loop(0, steps)
    def _(s):
        copy(s).start()

    make_tables(block, *tables)
    weigh.wait()
    weight = [weight_ref[e] for e in range(events)]

    @pl.loop(0, steps, step=SUM_UNROLL)
    def _(first):
        for u in range(SUM_UNROLL):
            s = first + u
            copy(s).wait()
            for r in range(rows):
                parts = []
                for h in range(halves):
                    total = weight[0] * landing[s, 0, h, r].astype(jnp.float32)
                    for e in range(1, events):
                        total = total + weight[e] * landing[s, e, h, r].astype(jnp.float32)
                    parts.append(total)
                turned[u, pl.ds(r, depth, stride=rows), :] = jnp.concatenate(parts, axis=0).T
            p, place = s // per_param, pl.multiple_of(lax.rem(s, per_param) * rows, rows)
            whole = turned[u].reshape(depth, rows, halves * width)
            out_ref[:, p, pl.ds(place, rows)] = whole.astype(out_ref.dtype)


def event_sum(kernels, event_weight, nx_all, ny_all):
    events, params, nx, ny, depth = kernels.shape
    halves = depth // ny
    rows = nx // halves
    split = kernels.reshape(events, params, halves, rows, ny, depth)
    tile, reach = TILE * nx, (TILE + 2 * MARGIN) * nx
    steps = params * rows // ROWS
    vmem = pl.BlockSpec(memory_space=pltpu.VMEM)
    hbm = pl.BlockSpec(memory_space=pltpu.HBM)
    return pl.pallas_call(
        functools.partial(sum_kernel, nx),
        in_specs=[hbm, hbm],
        out_specs=(vmem,) * 5,
        out_shape=(
            jax.ShapeDtypeStruct((depth, params, rows, halves * ny), jnp.bfloat16),
            jax.ShapeDtypeStruct((tile, reach), jnp.bfloat16),
            jax.ShapeDtypeStruct((reach, tile), jnp.bfloat16),
            jax.ShapeDtypeStruct((nx_all, depth), jnp.float32),
            jax.ShapeDtypeStruct((8, ny_all), jnp.float32),
        ),
        scratch_shapes=[
            pltpu.VMEM((steps, events, halves, ROWS, ny, depth), jnp.bfloat16),
            pltpu.SMEM((events,), jnp.float32),
            pltpu.VMEM((SUM_UNROLL, depth * ROWS, halves * ny), jnp.float32),
            pltpu.SemaphoreType.DMA((steps,)),
            pltpu.SemaphoreType.DMA,
        ],
        compiler_params=pltpu.CompilerParams(vmem_limit_bytes=SUM_MIB << 20),
        name="event_sum",
    )(pltpu.with_memory_space_constraint(event_weight, pltpu.HBM), split)


def smooth_kernel(size_y, block, in_ref, tile_ref, tile_t_ref, inv_x_ref, inv_y_ref, out_ref, plane):
    _, pairs, nx, pair = plane.shape
    ny = pairs * pair
    rows = in_ref.shape[2]
    tile, margin = tile_ref.shape[0], MARGIN * block
    swap_halves = lambda a, b: (
        jnp.concatenate([a[:, :block], b[:, :block]], axis=1),
        jnp.concatenate([a[:, block:], b[:, block:]], axis=1),
    )

    def build(p, i):
        for j in range(pairs):
            at = i * size_y + 2 * j
            upper, lower = swap_halves(in_ref[at, p], in_ref[at + 1, p])
            plane[p, j, i * block : i * block + rows] = upper
            plane[p, j, i * block + rows : (i + 1) * block] = lower

    def window(x0, x1):
        return max(0, x0 - REACH * block) // pair * pair, min(nx, -(-(x1 + REACH * block) // pair) * pair)

    def pack(p, x0, done):
        for i in range(done.shape[0] // block):
            for j in range(0, size_y, 2):
                part = done[i * block : (i + 1) * block, j * block : j * block + pair]
                at = (x0 // block + i) * size_y + j
                out_ref[at, p], out_ref[at + 1, p] = swap_halves(part[:rows], part[rows:])

    ends = [block * sum(X_TILES[:k]) for k in range(len(X_TILES) + 1)]
    assert ends[-1] == nx
    built = dict.fromkeys(range(in_ref.shape[1]), 0)

    def build_for(p, x0, x1):
        while built[p] * block < window(x0, x1)[1]:
            build(p, built[p])
            built[p] += 1

    def along_x(p, x0, x1):
        lo, hi = window(x0, x1)
        row = (x0 - lo) % pair
        col = margin + lo - x0 + row
        lines = jnp.concatenate([plane[p, j, lo:hi] for j in range(pairs)], axis=1)
        weights = tile_ref[row : row + x1 - x0, col : col + hi - lo]
        sums = jnp.dot(weights, lines, preferred_element_type=jnp.float32)
        inv_x = jnp.concatenate([inv_x_ref[x0:x1]] * (ny // inv_x_ref.shape[1]), axis=1)
        return (sums * inv_x).astype(jnp.bfloat16)

    def along_y(rows_in):
        parts = []
        for y0 in range(0, ny, tile):
            lo, hi = max(0, y0 - margin), min(ny, y0 + tile + margin)
            at = lo - (y0 - margin)
            sums = jnp.dot(rows_in[:, lo:hi], tile_t_ref[at : at + hi - lo], preferred_element_type=jnp.float32)
            parts.append((sums * inv_y_ref[0:1, y0 : y0 + tile]).astype(jnp.bfloat16))
        return jnp.concatenate(parts, axis=1)

    tiles = list(zip(ends, ends[1:]))
    params = in_ref.shape[1]
    for x0, x1 in tiles:
        build_for(0, x0, x1)
    last = None
    for p in range(params):
        mixed = jnp.concatenate([along_x(p, x0, x1) for x0, x1 in tiles], axis=0)
        if p + 1 < params:
            for x0, x1 in tiles:
                build_for(p + 1, x0, x1)
        if last is not None:
            pack(p - 1, 0, last)
        last = along_y(mixed)
    pack(params - 1, 0, last)


def smooth(lines, block, size_x, size_y, tables):
    blocks, params, rows, width = lines.shape
    nx = size_x * block
    whole = lambda a: pl.BlockSpec(a.shape, lambda p: (0,) * a.ndim)
    spec = pl.BlockSpec((blocks, PLANES, rows, width), lambda p: (0, p, 0, 0))
    return pl.pallas_call(
        functools.partial(smooth_kernel, size_y, block),
        grid=(params // PLANES,),
        in_specs=[spec] + [whole(t) for t in tables],
        out_specs=spec,
        out_shape=jax.ShapeDtypeStruct(lines.shape, jnp.bfloat16),
        scratch_shapes=[pltpu.VMEM((PLANES, size_y // 2, nx, 2 * block), jnp.bfloat16)],
        compiler_params=pltpu.CompilerParams(vmem_limit_bytes=SMOOTH_MIB << 20),
        name="smooth",
    )(lines, *tables)


def turn_kernel(in_ref, out_ref, leaving, wide, left):
    steps, halves, rows, width, _ = leaving.shape
    depth, params, _, pair = in_ref.shape
    per_param = steps // params

    def copy(s):
        p, r = s // per_param, lax.rem(s, per_param)
        return pltpu.make_async_copy(leaving.at[s], out_ref.at[p, :, pl.ds(r * rows, rows)], left.at[s])

    @pl.loop(0, steps, step=TURN_UNROLL)
    def _(first):
        for u in range(TURN_UNROLL):
            s = first + u
            p, place = s // per_param, pl.multiple_of(lax.rem(s, per_param) * rows, rows)
            wide[u] = in_ref[:, p, pl.ds(place, rows)].astype(jnp.float32).reshape(depth * rows, pair)
            for r in range(rows):
                turned = wide[u, pl.ds(r, depth, stride=rows), :].T
                for h in range(halves):
                    leaving[s, h, r] = turned[h * width : (h + 1) * width]
            copy(s).start()

    @pl.loop(0, steps)
    def _(s):
        copy(s).wait()


def turn_back(done, block):
    depth, params, rows, pair = done.shape
    halves = pair // block
    steps = params * rows // ROWS
    out = pl.pallas_call(
        turn_kernel,
        in_specs=[pl.BlockSpec(memory_space=pltpu.VMEM)],
        out_specs=pl.BlockSpec(memory_space=pl.ANY),
        out_shape=jax.ShapeDtypeStruct((params, halves, rows, block, depth), jnp.float32),
        scratch_shapes=[
            pltpu.VMEM((steps, halves, ROWS, block, depth), jnp.float32),
            pltpu.VMEM((TURN_UNROLL, depth * ROWS, pair), jnp.float32),
            pltpu.SemaphoreType.DMA((steps,)),
        ],
        compiler_params=pltpu.CompilerParams(vmem_limit_bytes=24 << 20),
        name="turn_back",
    )(done)
    return out.reshape(params, halves * rows, block, depth)


def body(kernels, event_weight):
    block = kernels.shape[2]
    size_x, size_y = lax.axis_size("gx"), lax.axis_size("gy")
    summed, *tables = event_sum(kernels, event_weight, size_x * block, size_y * block)
    swap = functools.partial(lax.all_to_all, axis_name=AXES, split_axis=0, concat_axis=0, tiled=True)
    done = smooth(swap(summed), block, size_x, size_y, tables)
    return turn_back(swap(done), block)


def solution(mesh):
    return jax.shard_map(
        body,
        mesh=mesh,
        in_specs=(P(None, None, "gx", "gy", None), P()),
        out_specs=P(None, "gx", "gy", None),
        check_vma=False,
    )
```

```python
import functools
import jax
import jax.numpy as jnp
from jax import lax
from jax.experimental import pallas as pl
from jax.experimental.pallas import tpu as pltpu
from jax.sharding import PartitionSpec as P

REACH = 3
MARGIN = 4
AXES = ("gx", "gy")
TILE = 8
X_TILES = (5, 6, 5)
SUM_MIB = 36
SMOOTH_MIB = 24
LAST_PARTS = 2
PLANES = 4
SUM_UNROLL = 2
TURN_UNROLL = 16
ROWS = 8


def gauss_weights(offsets, radius, sigma):
    values = offsets.astype(jnp.float32)
    weights = jnp.exp(-values * values / (2.0 * sigma * sigma))
    return jnp.where(jnp.abs(offsets) <= radius, weights, 0.0).astype(jnp.bfloat16)


def band(rows, cols, shift, axis, sigma, radius):
    far = lax.broadcasted_iota(jnp.int32, (rows, cols), axis)
    near = lax.broadcasted_iota(jnp.int32, (rows, cols), 1 - axis)
    return gauss_weights(far - near - shift, radius, sigma)


def clipped(first, window, margin, total):
    return max(0, margin - first), min(window, total - first + margin)


def make_tables(block, tile_ref, tile_t_ref, inv_x_ref, inv_y_ref):
    radius, sigma, margin = REACH * block, 2.0 * block, MARGIN * block
    step = 2 * block
    window = step + 2 * margin
    weights = band(step, window, margin, 1, sigma, radius)
    weights_t = band(window, step, margin, 0, sigma, radius)
    tile, reach = tile_ref.shape
    for at in range(0, tile, step):
        own = slice(at, at + step)
        tile_ref[own, at : at + window] = weights
        tile_t_ref[at : at + window, own] = weights_t
        for lo, hi in ((0, at), (at + window, reach)):
            if hi > lo:
                tile_ref[own, lo:hi] = jnp.zeros((step, hi - lo), tile_ref.dtype)
                tile_t_ref[lo:hi, own] = jnp.zeros((hi - lo, step), tile_t_ref.dtype)
    nx, ny = inv_x_ref.shape[0], inv_y_ref.shape[1]
    wide, wide_t = weights.astype(jnp.float32), weights_t.astype(jnp.float32)
    for x0 in range(0, nx, step):
        lo, hi = clipped(x0, window, margin, nx)
        sums = jnp.sum(wide[:, lo:hi], axis=1, keepdims=True)
        inv_x_ref[x0 : x0 + step] = jnp.broadcast_to(1.0 / sums, (step, inv_x_ref.shape[1]))
    for y0 in range(0, ny, step):
        lo, hi = clipped(y0, window, margin, ny)
        sums = jnp.sum(wide_t[lo:hi], axis=0, keepdims=True)
        inv_y_ref[:, y0 : y0 + step] = jnp.broadcast_to(1.0 / sums, (inv_y_ref.shape[0], step))


def sum_kernel(block, weight_hbm, kernels_ref, out_ref, *refs):
    tables, (landing, weight_ref, turned, arrived, weighed) = refs[:4], refs[4:]
    steps, events, halves, rows, width, depth = landing.shape
    per_param = steps // kernels_ref.shape[1]

    def copy(s):
        p, r = s // per_param, lax.rem(s, per_param)
        return pltpu.make_async_copy(
            kernels_ref.at[:, p, :, pl.ds(r * rows, rows)], landing.at[s], arrived.at[s]
        )

    weigh = pltpu.make_async_copy(weight_hbm, weight_ref, weighed)
    weigh.start()

    @pl.loop(0, steps)
    def _(s):
        copy(s).start()

    make_tables(block, *tables)
    weigh.wait()
    weight = [weight_ref[e] for e in range(events)]

    @pl.loop(0, steps, step=SUM_UNROLL)
    def _(first):
        for u in range(SUM_UNROLL):
            s = first + u
            copy(s).wait()
            for r in range(rows):
                parts = []
                for h in range(halves):
                    total = weight[0] * landing[s, 0, h, r].astype(jnp.float32)
                    for e in range(1, events):
                        total = total + weight[e] * landing[s, e, h, r].astype(jnp.float32)
                    parts.append(total)
                turned[u, pl.ds(r, depth, stride=rows), :] = jnp.concatenate(parts, axis=0).T
            p, place = s // per_param, pl.multiple_of(lax.rem(s, per_param) * rows, rows)
            whole = turned[u].reshape(depth, rows, halves * width)
            out_ref[:, p, pl.ds(place, rows)] = whole.astype(out_ref.dtype)


def event_sum(kernels, event_weight, nx_all, ny_all):
    events, params, nx, ny, depth = kernels.shape
    halves = depth // ny
    rows = nx // halves
    split = kernels.reshape(events, params, halves, rows, ny, depth)
    tile, reach = TILE * nx, (TILE + 2 * MARGIN) * nx
    steps = params * rows // ROWS
    vmem = pl.BlockSpec(memory_space=pltpu.VMEM)
    hbm = pl.BlockSpec(memory_space=pltpu.HBM)
    return pl.pallas_call(
        functools.partial(sum_kernel, nx),
        in_specs=[hbm, hbm],
        out_specs=(vmem,) * 5,
        out_shape=(
            jax.ShapeDtypeStruct((depth, params, rows, halves * ny), jnp.bfloat16),
            jax.ShapeDtypeStruct((tile, reach), jnp.bfloat16),
            jax.ShapeDtypeStruct((reach, tile), jnp.bfloat16),
            jax.ShapeDtypeStruct((nx_all, depth), jnp.float32),
            jax.ShapeDtypeStruct((8, ny_all), jnp.float32),
        ),
        scratch_shapes=[
            pltpu.VMEM((steps, events, halves, ROWS, ny, depth), jnp.bfloat16),
            pltpu.SMEM((events,), jnp.float32),
            pltpu.VMEM((SUM_UNROLL, depth * ROWS, halves * ny), jnp.float32),
            pltpu.SemaphoreType.DMA((steps,)),
            pltpu.SemaphoreType.DMA,
        ],
        compiler_params=pltpu.CompilerParams(vmem_limit_bytes=SUM_MIB << 20),
        name="event_sum",
    )(pltpu.with_memory_space_constraint(event_weight, pltpu.HBM), split)


def smooth_kernel(size_y, block, in_ref, tile_ref, tile_t_ref, inv_x_ref, inv_y_ref, out_ref, plane):
    _, pairs, nx, pair = plane.shape
    ny = pairs * pair
    rows = in_ref.shape[2]
    tile, margin = tile_ref.shape[0], MARGIN * block
    swap_halves = lambda a, b: (
        jnp.concatenate([a[:, :block], b[:, :block]], axis=1),
        jnp.concatenate([a[:, block:], b[:, block:]], axis=1),
    )

    def build(p, i):
        for j in range(pairs):
            at = i * size_y + 2 * j
            upper, lower = swap_halves(in_ref[at, p], in_ref[at + 1, p])
            plane[p, j, i * block : i * block + rows] = upper
            plane[p, j, i * block + rows : (i + 1) * block] = lower

    def window(x0, x1):
        return max(0, x0 - REACH * block) // pair * pair, min(nx, -(-(x1 + REACH * block) // pair) * pair)

    def pack(p, x0, done):
        for i in range(done.shape[0] // block):
            for j in range(0, size_y, 2):
                part = done[i * block : (i + 1) * block, j * block : j * block + pair]
                at = (x0 // block + i) * size_y + j
                out_ref[at, p], out_ref[at + 1, p] = swap_halves(part[:rows], part[rows:])

    ends = [block * sum(X_TILES[:k]) for k in range(len(X_TILES) + 1)]
    assert ends[-1] == nx
    built = dict.fromkeys(range(in_ref.shape[1]), 0)

    def build_for(p, x0, x1):
        while built[p] * block < window(x0, x1)[1]:
            build(p, built[p])
            built[p] += 1

    def along_x(p, x0, x1):
        lo, hi = window(x0, x1)
        row = (x0 - lo) % pair
        col = margin + lo - x0 + row
        lines = jnp.concatenate([plane[p, j, lo:hi] for j in range(pairs)], axis=1)
        weights = tile_ref[row : row + x1 - x0, col : col + hi - lo]
        sums = jnp.dot(weights, lines, preferred_element_type=jnp.float32)
        inv_x = jnp.concatenate([inv_x_ref[x0:x1]] * (ny // inv_x_ref.shape[1]), axis=1)
        return (sums * inv_x).astype(jnp.bfloat16)

    def along_y(rows_in):
        parts = []
        for y0 in range(0, ny, tile):
            lo, hi = max(0, y0 - margin), min(ny, y0 + tile + margin)
            at = lo - (y0 - margin)
            sums = jnp.dot(rows_in[:, lo:hi], tile_t_ref[at : at + hi - lo], preferred_element_type=jnp.float32)
            parts.append((sums * inv_y_ref[0:1, y0 : y0 + tile]).astype(jnp.bfloat16))
        return jnp.concatenate(parts, axis=1)

    tiles = list(zip(ends, ends[1:]))
    params = in_ref.shape[1]
    last = None
    for p in range(params):
        mixed = []
        for x0, x1 in tiles:
            build_for(p, x0, x1)
            mixed.append(along_x(p, x0, x1))
        mixed = jnp.concatenate(mixed, axis=0)
        if p + 1 < params:
            for x0, x1 in tiles:
                build_for(p + 1, x0, x1)
        if last is not None:
            pack(p - 1, 0, last)
        if p + 1 < params:
            last = along_y(mixed)
    part = nx // LAST_PARTS
    ready = None
    for x0 in range(0, nx, part):
        done = along_y(mixed[x0 : x0 + part])
        if ready is not None:
            pack(params - 1, x0 - part, ready)
        ready = done
    pack(params - 1, nx - part, ready)


def smooth(lines, block, size_x, size_y, tables):
    blocks, params, rows, width = lines.shape
    nx = size_x * block
    whole = lambda a: pl.BlockSpec(a.shape, lambda p: (0,) * a.ndim)
    spec = pl.BlockSpec((blocks, PLANES, rows, width), lambda p: (0, p, 0, 0))
    return pl.pallas_call(
        functools.partial(smooth_kernel, size_y, block),
        grid=(params // PLANES,),
        in_specs=[spec] + [whole(t) for t in tables],
        out_specs=spec,
        out_shape=jax.ShapeDtypeStruct(lines.shape, jnp.bfloat16),
        scratch_shapes=[pltpu.VMEM((PLANES, size_y // 2, nx, 2 * block), jnp.bfloat16)],
        compiler_params=pltpu.CompilerParams(vmem_limit_bytes=SMOOTH_MIB << 20),
        name="smooth",
    )(lines, *tables)


def turn_kernel(in_ref, out_ref, leaving, wide, left):
    steps, halves, rows, width, _ = leaving.shape
    depth, params, _, pair = in_ref.shape
    per_param = steps // params

    def copy(s):
        p, r = s // per_param, lax.rem(s, per_param)
        return pltpu.make_async_copy(leaving.at[s], out_ref.at[p, :, pl.ds(r * rows, rows)], left.at[s])

    @pl.loop(0, steps, step=TURN_UNROLL)
    def _(first):
        for u in range(TURN_UNROLL):
            s = first + u
            p, place = s // per_param, pl.multiple_of(lax.rem(s, per_param) * rows, rows)
            wide[u] = in_ref[:, p, pl.ds(place, rows)].astype(jnp.float32).reshape(depth * rows, pair)
            for r in range(rows):
                turned = wide[u, pl.ds(r, depth, stride=rows), :].T
                for h in range(halves):
                    leaving[s, h, r] = turned[h * width : (h + 1) * width]
            copy(s).start(priority=u % 2)

    @pl.loop(0, steps)
    def _(s):
        copy(s).wait()


def turn_back(done, block):
    depth, params, rows, pair = done.shape
    halves = pair // block
    steps = params * rows // ROWS
    out = pl.pallas_call(
        turn_kernel,
        in_specs=[pl.BlockSpec(memory_space=pltpu.VMEM)],
        out_specs=pl.BlockSpec(memory_space=pl.ANY),
        out_shape=jax.ShapeDtypeStruct((params, halves, rows, block, depth), jnp.float32),
        scratch_shapes=[
            pltpu.VMEM((steps, halves, ROWS, block, depth), jnp.float32),
            pltpu.VMEM((TURN_UNROLL, depth * ROWS, pair), jnp.float32),
            pltpu.SemaphoreType.DMA((steps,)),
        ],
        compiler_params=pltpu.CompilerParams(vmem_limit_bytes=24 << 20),
        name="turn_back",
    )(done)
    return out.reshape(params, halves * rows, block, depth)


def body(kernels, event_weight):
    block = kernels.shape[2]
    size_x, size_y = lax.axis_size("gx"), lax.axis_size("gy")
    summed, *tables = event_sum(kernels, event_weight, size_x * block, size_y * block)
    swap = functools.partial(lax.all_to_all, axis_name=AXES, split_axis=0, concat_axis=0, tiled=True)
    done = smooth(swap(summed), block, size_x, size_y, tables)
    return turn_back(swap(done), block)


def solution(mesh):
    return jax.shard_map(
        body,
        mesh=mesh,
        in_specs=(P(None, None, "gx", "gy", None), P()),
        out_specs=P(None, "gx", "gy", None),
        check_vma=False,
    )
```
